512 devices in a mesh: row: 64 (over y, z), col: 8 (over x, core).
Axes of the slice: x: 4, y: 8, z: 8, core: 2. Of those that a mesh axis runs over, the one named last changes fastest.
Arguments:
- new_aux: bfloat16 [8192, 4096], P('row', 'col'), may hold values from -6 to 6
- former_auxiliary_rows: bfloat16 [81920, 4096], P('row', 'col'), may hold values from -6 to 6
- old_emb: bfloat16 [81920, 4096], P('row', 'col'), may hold values from -6 to 6
- neighbour_ids: int32 [8192, 16], P('row'), may hold values from -1 to 81919, as said below
- neighbour_counts: int32 [8192], P('row'), may hold values from 8 to 16
Outputs:
- new_emb: bfloat16 [8192, 4096], P('row', 'col')
The draws below stay inside these ranges and needn't reach their ends.
Inputs may be any that keep to these rules, and one draw needn't show every extreme that they name: neighbour_ids[j, k] is an old row number for k < neighbour_counts[j] and -1 otherwise. The live entries of the 128 new rows of one index of row name at most 48 entries, and at most 24 different rows, within one block of 1280 old rows held by one index of row; both bounds are reached in every draw.
All inputs are finite; a program needn't handle non-finite values.
Results may differ from the reference program's by a relative error of at most 0.0049.
Values may be sent and summed in bfloat16 or wider, within the bound.
A program may use at most 64 MiB of HBM per device.

```python
import jax
import jax.numpy as jnp
from jax import lax

D = 4096
OLD_DEV = 1280
NEW_DEV = 128
NEIGHBOURS = 16
OLD_ROWS = 81920
FRESH_ROW_COUNT = 8192
CAPACITY = 48
DISTINCT = 24
N_ROW = 64


def adjacent_lookup_lists(key):
    counts = jax.random.randint(jax.random.fold_in(key, 11), (FRESH_ROW_COUNT,), 8, NEIGHBOURS + 1).astype(jnp.int32)
    admissible_flags = jnp.arange(NEIGHBOURS, dtype=jnp.int32)[None, :] < counts[:, None]
    live_blocks = admissible_flags.reshape(N_ROW, NEW_DEV * NEIGHBOURS)
    ranks = jnp.cumsum(live_blocks.astype(jnp.int32), axis=1) - 1
    total = N_ROW * CAPACITY
    sharpest_weighting = jax.random.randint(jax.random.fold_in(key, 12), (), 0, N_ROW).astype(jnp.int32)
    order_keys = jax.random.split(jax.random.fold_in(key, 13), N_ROW)
    positions = jax.vmap(lambda k: jax.random.permutation(k, total))(order_keys).astype(jnp.int32)
    slot_owner = jnp.arange(total, dtype=jnp.int32) // CAPACITY
    priority = jnp.where(slot_owner == sharpest_weighting, 0, total)[None, :].astype(jnp.int32) + positions
    order = jnp.argsort(priority, axis=1).astype(jnp.int32)
    slots = jnp.take_along_axis(order, jnp.clip(ranks, 0, total - 1), axis=1)
    owners = slots // CAPACITY
    within = slots % CAPACITY % DISTINCT
    pool_keys = jax.random.split(jax.random.fold_in(key, 14), N_ROW * N_ROW)
    pools = jax.vmap(lambda k: jax.random.permutation(k, OLD_DEV)[:DISTINCT])(pool_keys).astype(jnp.int32)
    pools = pools.reshape(N_ROW, N_ROW, DISTINCT)
    block_index = jnp.arange(N_ROW, dtype=jnp.int32)[:, None]
    local_rows = pools[block_index, owners, within]
    numbers = owners * OLD_DEV + local_rows
    numbers = jnp.where(live_blocks, numbers, -1).reshape(FRESH_ROW_COUNT, NEIGHBOURS).astype(jnp.int32)
    return (numbers, counts)


def draw_neighbour_ids(key, part):
    return adjacent_lookup_lists(key)[0]


def draw_neighbour_counts(key, part):
    return adjacent_lookup_lists(key)[1]


def level_of(own_key, dims, shards, smallest, high):
    def one(dim, parts):
        draws = jax.random.uniform(jax.random.fold_in(jax.random.fold_in(own_key, 6), dim), (parts,), jnp.float32, smallest / len(shards), high / len(shards))
        return jnp.repeat(jnp.exp(draws), dims[dim] // parts).reshape((-1,) + (1,) * (len(dims) - dim - 1))

    loudness = one(*shards[0])
    for cut in shards[1:]:
        loudness = loudness * one(*cut)
    return loudness


def gaussian(stream_key, dims, spread, bound, cuts=(), held_as=jnp.bfloat16):
    result = spread * jax.random.normal(stream_key, dims, jnp.float32)
    if cuts:
        result = result * level_of(stream_key, dims, cuts, -0.22, 0.18)
    return jnp.clip(result, -bound, bound).astype(held_as)


def setup_inputs(seed: int = 0) -> dict:
    keys = jax.random.split(jax.random.key(seed), 6)
    return {
        "new_aux": gaussian(keys[0], (FRESH_ROW_COUNT, D), 1.0, 6.0, ((0, 64), (1, 8))),
        "former_auxiliary_rows": gaussian(keys[1], (OLD_ROWS, D), 1.0, 6.0, ((0, 64), (1, 8))),
        "old_emb": gaussian(keys[2], (OLD_ROWS, D), 1.0, 6.0, ((0, 64), (1, 8))),
        "neighbour_ids": draw_neighbour_ids(jax.random.fold_in(keys[5], 71), 0),
        "neighbour_counts": draw_neighbour_counts(jax.random.fold_in(keys[5], 71), 0),
    }


eps = 1e-06
exponential_sharpness = 0.025

def blend_block(args):
    former_auxiliary_rows, old_emb, aux_block, neighbour_index_block, admissible_flag_tile = args
    near_aux = former_auxiliary_rows[neighbour_index_block].astype(jnp.float32)
    near_emb = old_emb[neighbour_index_block].astype(jnp.float32)
    own = aux_block.astype(jnp.float32)
    inner = jnp.einsum('jd,jkd->jk', own, near_aux)
    near_sq = jnp.einsum('jkd,jkd->jk', near_aux, near_aux)
    own_sq = jnp.einsum('jd,jd->j', own, own)
    angular_similarity_values = inner * lax.rsqrt((own_sq[:, None] + eps) * (near_sq + eps))
    plain_affinity_values = jnp.where(admissible_flag_tile, jnp.exp(angular_similarity_values / exponential_sharpness), jnp.float32(0.0))
    weights = (plain_affinity_values / lax.optimization_barrier(jnp.sum(plain_affinity_values, axis=1, keepdims=True))).astype(jnp.bfloat16)
    blended = jnp.einsum('jk,jkd->jd', weights.astype(jnp.float32), near_emb)
    return blended.astype(jnp.bfloat16)

def reference(new_aux, former_auxiliary_rows, old_emb, neighbour_ids, neighbour_counts):
    admissible_flags = jnp.arange(NEIGHBOURS, dtype=jnp.int32)[None, :] < neighbour_counts[:, None]
    safe = jnp.where(admissible_flags, neighbour_ids, 0).astype(jnp.int32)

    def one(args):
        aux_block, neighbour_index_block, admissible_flag_tile = args
        return blend_block((former_auxiliary_rows, old_emb, aux_block, neighbour_index_block, admissible_flag_tile))
    blocks = lax.map(one, (new_aux.reshape(N_ROW, NEW_DEV, D), safe.reshape(N_ROW, NEW_DEV, NEIGHBOURS), admissible_flags.reshape(N_ROW, NEW_DEV, NEIGHBOURS)))
    return blocks.reshape(FRESH_ROW_COUNT, D)
```

```python
import functools

import jax
import jax.numpy as jnp
from jax import lax
from jax.experimental import pallas as pl
from jax.experimental.pallas import tpu as pltpu
from jax.sharding import PartitionSpec as P

MESH = pl.DeviceIdType.MESH
F32, BF16, I32 = jnp.float32, jnp.bfloat16, jnp.int32
DISTINCT = 24
SIDE = 8
LANES = 128
eps = 1e-06
exponential_sharpness = 0.025


def iota(shape, dim):
    return lax.broadcasted_iota(I32, shape, dim)


def kernel(n_row, n_col, ids_ref, cnt_ref, new_ref, aux_hbm, emb_hbm, out_ref,
           aux_tab, emb_tab, row_hot, lo_hot, ranks, lists, asked, sel, send_aux, send_emb,
           got_aux, got_emb, slot_wide, w_wide, w_slots, part, parts,
           tab_sem, list_send, list_recv, aux_send, aux_recv, emb_send, emb_recv, part_send, part_recv):
    slots_row, new_dev = ids_ref.shape
    old_dev, width = aux_hbm.shape
    his = old_dev // LANES
    me = lax.axis_index("row")
    my_col = lax.axis_index("col")
    y, z = me // SIDE, me % SIDE

    def shift(i):
        p, q = i % SIDE, i // SIDE
        return (3 * p) % SIDE, (3 * q + p) % SIDE

    def asker(i):
        dy, dz = shift(i)
        return ((y + dy) % SIDE) * SIDE + (z + dz) % SIDE

    def owner(i):
        dy, dz = shift(i)
        return ((y - dy + SIDE) % SIDE) * SIDE + (z - dz + SIDE) % SIDE

    tabs = [pltpu.make_async_copy(aux_hbm, aux_tab, tab_sem.at[0]),
            pltpu.make_async_copy(emb_hbm, emb_tab, tab_sem.at[1])]
    for t in tabs:
        t.start()

    barrier = pltpu.get_barrier_semaphore()

    def greet(i, c):
        pl.semaphore_signal(barrier, inc=1, device_id={"row": asker(i)}, device_id_type=MESH)
        return c
    lax.fori_loop(1, n_row, greet, 0)
    for c in range(1, n_col):
        pl.semaphore_signal(barrier, inc=1, device_id={"col": (my_col + c) % n_col}, device_id_type=MESH)

    ids = ids_ref[...]
    live = iota(ids.shape, 0) < cnt_ref[...]
    group = jnp.where(live, ids, 0) >> 7
    lo = ids & (LANES - 1)
    own = (group * 205) >> 11
    hi = group - his * own
    at = jnp.where(live, hi * n_row + own, -1)
    sub_all = iota((his * n_row, new_dev), 0)
    sub_lo = iota((LANES, new_dev), 0)
    for k in range(slots_row):
        cols = slice(k * new_dev, (k + 1) * new_dev)
        row_hot[:, cols] = jnp.where(sub_all == at[k:k + 1, :], 1.0, 0.0).astype(BF16)
        lo_hot[:, cols] = jnp.where(sub_lo == lo[k:k + 1, :], 1.0, 0.0).astype(BF16)
    named = lax.dot_general(row_hot[...], lo_hot[...], (((1,), (1,)), ((), ())), preferred_element_type=F32)
    present = named > 0.5
    mask = jnp.where(present, 1.0, 0.0).astype(BF16)
    i0, i1 = iota((LANES, LANES), 0), iota((LANES, LANES), 1)
    before = jnp.dot(mask, jnp.where(i0 < i1, 1.0, 0.0).astype(BF16), preferred_element_type=F32)
    per_row = jnp.dot(mask, jnp.ones((LANES, LANES), BF16), preferred_element_type=F32)
    ahead = jnp.zeros((n_row, LANES), F32)
    for h in range(his):
        rows = slice(h * n_row, (h + 1) * n_row)
        ranks[rows, :] = jnp.where(present[rows], before[rows] + ahead, -1.0)
        ahead = ahead + per_row[rows]

    lane = iota((n_row, LANES), 1)
    lane_f = lane.astype(F32)
    table = jnp.zeros((n_row, LANES), F32)
    for c in range(DISTINCT):
        acc = jnp.zeros((n_row, LANES), F32)
        for h in range(his):
            acc = acc + jnp.where(ranks[h * n_row:(h + 1) * n_row, :] == float(c), lane_f + float(h * LANES), 0.0)
        table = jnp.where(lane == c, jnp.sum(acc, axis=1, keepdims=True), table)
    for o in range(n_row):
        lists[o] = table[o:o + 1, :]

    pl.semaphore_wait(barrier, n_row - 1 + n_col - 1)

    groups = list_recv.shape[0]
    per = n_row // groups
    pltpu.make_async_copy(lists.at[me], asked.at[0], list_recv.at[0]).start()

    def ask(i, c):
        pltpu.make_async_remote_copy(
            lists.at[me * 0 + owner(i)], asked.at[i], list_send, list_recv.at[i // per],
            device_id={"row": owner(i)}, device_id_type=MESH).start()
        return c
    lax.fori_loop(1, n_row, ask, 0)

    for t in tabs:
        t.wait()

    wide = iota((DISTINCT, old_dev), 1).astype(F32)

    def send(src, dst, s_sem, r_sem, i):
        return pltpu.make_async_remote_copy(src.at[i], dst.at[me], s_sem, r_sem,
                                            device_id={"row": asker(i)}, device_id_type=MESH)

    def put(g, tab, src, dst, s_sem, r_sem):
        rows = jnp.dot(sel[g * per * DISTINCT:(g + 1) * per * DISTINCT, :], tab[...], preferred_element_type=F32)
        for a in range(per):
            src[g * per + a] = rows[a * DISTINCT:(a + 1) * DISTINCT].astype(BF16)
        if g == 0:
            pltpu.make_async_copy(src.at[0], dst.at[me], r_sem).start()

        def go(i, c):
            send(src, dst, s_sem, r_sem, i).start()
            return c
        lax.fori_loop(max(g * per, 1), (g + 1) * per, go, 0)

    for g in range(groups):
        pltpu.make_async_copy(asked.at[pl.ds(g * per, per)], asked.at[pl.ds(g * per, per)], list_recv.at[g]).wait()
        want = jnp.concatenate([asked[g * per + a] for a in range(per)], axis=0).T
        for a in range(0, per, 2):
            pair = jnp.concatenate(
                [jnp.where(want[:DISTINCT, b:b + 1] == wide, 1.0, 0.0) for b in (a, a + 1)], axis=0)
            sel[(g * per + a) * DISTINCT:(g * per + a + 2) * DISTINCT, :] = pair.astype(BF16)
        put(g, aux_tab, send_aux, got_aux, aux_send, aux_recv)
    for g in range(groups):
        put(g, emb_tab, send_emb, got_emb, emb_send, emb_recv)

    found = lax.dot_general(ranks[...].astype(BF16), row_hot[...], (((0,), (0,)), ((), ())), preferred_element_type=F32)
    for k in range(slots_row):
        cols = slice(k * new_dev, (k + 1) * new_dev)
        pos = jnp.sum(jnp.where(sub_lo == lo[k:k + 1, :], found[:, cols], 0.0), axis=0, keepdims=True)
        slot = jnp.where(live[k:k + 1, :], own[k:k + 1, :] * DISTINCT + pos.astype(I32), -1)
        slot_wide[k] = jnp.broadcast_to(slot, (8, new_dev))

    new = new_ref[...]
    own_sq = jnp.sum(jnp.square(new.astype(F32)), axis=1, keepdims=True)
    own_sq = jnp.broadcast_to(own_sq, (new_dev, LANES)).T[0:8, :]

    pltpu.make_async_copy(got_aux, got_aux, aux_recv).wait()

    sub8 = iota((8, new_dev), 0)

    def inner_step(o, acc):
        rows = got_aux[o]
        prod = lax.dot_general(rows, new, (((1,), (1,)), ((), ())), preferred_element_type=F32)
        near = jnp.broadcast_to(jnp.sum(jnp.square(rows.astype(F32)), axis=1, keepdims=True), (DISTINCT, new_dev))
        acc = list(acc)
        for t in range(DISTINCT // 8):
            here = sub8 + (o * DISTINCT + 8 * t)
            for k in range(slots_row):
                hit = slot_wide[k] == here
                acc[k] = acc[k] + jnp.where(hit, prod[8 * t:8 * t + 8], 0.0)
                acc[slots_row + k] = acc[slots_row + k] + jnp.where(hit, near[8 * t:8 * t + 8], 0.0)
        return tuple(acc)

    acc = lax.fori_loop(0, n_row, inner_step, tuple(jnp.zeros((8, new_dev), F32) for _ in range(2 * slots_row)))
    for k in range(2 * slots_row):
        part[k:k + 1, :] = jnp.sum(acc[k], axis=0, keepdims=True)
    part[2 * slots_row:2 * slots_row + 8, :] = own_sq

    for c in range(1, n_col):
        pltpu.make_async_remote_copy(part, parts.at[c - 1], part_send.at[c - 1], part_recv.at[c - 1],
                                     device_id={"col": (my_col + c) % n_col}, device_id_type=MESH).start()
    total = part[...]
    for c in range(1, n_col):
        pltpu.make_async_copy(part, parts.at[c - 1], part_recv.at[c - 1]).wait()
        total = total + parts[c - 1]

    inner, near_sq = total[:slots_row], total[slots_row:2 * slots_row]
    own_all = total[2 * slots_row:2 * slots_row + 1]
    similarity = inner * lax.rsqrt((own_all + eps) * (near_sq + eps))
    raw = jnp.where(live, jnp.exp(similarity / exponential_sharpness), 0.0)
    weights = (raw / jnp.sum(raw, axis=0, keepdims=True)).astype(BF16).astype(F32)
    for k in range(slots_row):
        w_wide[k] = jnp.broadcast_to(weights[k:k + 1, :], (8, new_dev))

    def weigh(o, c):
        for t in range(DISTINCT // 8):
            start = pl.multiple_of(o * DISTINCT + 8 * t, 8)
            here = sub8 + start
            acc = jnp.zeros((8, new_dev), F32)
            for k in range(slots_row):
                acc = acc + jnp.where(slot_wide[k] == here, w_wide[k], 0.0)
            w_slots[pl.ds(start, 8), :] = acc
        return c
    lax.fori_loop(0, n_row, weigh, 0)
    w_t = w_slots[...].T.astype(BF16)

    pltpu.make_async_copy(got_emb, got_emb, emb_recv).wait()
    near_emb = got_emb[...].reshape(n_row * DISTINCT, width)
    out_ref[...] = jnp.dot(w_t, near_emb, preferred_element_type=F32).astype(BF16)

    rest = pl.ds(0, n_row - 1)
    pltpu.make_async_copy(lists.at[rest], lists.at[rest], list_send).wait()
    pltpu.make_async_copy(send_aux.at[rest], send_aux.at[rest], aux_send).wait()
    pltpu.make_async_copy(send_emb.at[rest], send_emb.at[rest], emb_send).wait()
    for c in range(1, n_col):
        pltpu.make_async_copy(part, part, part_send.at[c - 1]).wait()


def solution(mesh):
    n_row, n_col = mesh.shape["row"], mesh.shape["col"]

    def local(new_aux, former_auxiliary_rows, old_emb, neighbour_ids, neighbour_counts):
        new_dev, width = new_aux.shape
        old_dev = former_auxiliary_rows.shape[0]
        slots_row = neighbour_ids.shape[1]
        slots = n_row * DISTINCT
        his = old_dev // LANES
        vm = pltpu.VMEM
        dma = pltpu.SemaphoreType.DMA
        spec = pl.BlockSpec(memory_space=vm)
        hbm = pl.BlockSpec(memory_space=pl.ANY)
        return pl.pallas_call(
            functools.partial(kernel, n_row, n_col),
            out_shape=jax.ShapeDtypeStruct((new_dev, width), BF16),
            in_specs=[spec, spec, spec, hbm, hbm],
            out_specs=spec,
            scratch_shapes=[
                vm((old_dev, width), BF16), vm((old_dev, width), BF16),
                vm((his * n_row, slots_row * new_dev), BF16), vm((LANES, slots_row * new_dev), BF16),
                vm((his * n_row, LANES), F32), vm((n_row, 1, LANES), F32), vm((n_row, 1, LANES), F32),
                vm((slots, old_dev), BF16),
                vm((n_row, DISTINCT, width), BF16), vm((n_row, DISTINCT, width), BF16),
                vm((n_row, DISTINCT, width), BF16), vm((n_row, DISTINCT, width), BF16),

                vm((slots_row, 8, new_dev), I32), vm((slots_row, 8, new_dev), F32),
                vm((slots, new_dev), F32),
                vm((2 * slots_row + 8, new_dev), F32), vm((n_col - 1, 2 * slots_row + 8, new_dev), F32),
                dma((2,)), dma(()), dma((4,)), dma(()), dma(()), dma(()), dma(()),
                dma((n_col - 1,)), dma((n_col - 1,)),
            ],
            compiler_params=pltpu.CompilerParams(
                collective_id=0, has_side_effects=True, vmem_limit_bytes=48 * 1024 * 1024),
        )(neighbour_ids.T, neighbour_counts.reshape(1, new_dev), new_aux, former_auxiliary_rows, old_emb)

    return jax.shard_map(
        local,
        mesh=mesh,
        in_specs=(P("row", "col"), P("row", "col"), P("row", "col"), P("row", None), P("row")),
        out_specs=P("row", "col"),
        check_vma=False,
    )
```

```python
import functools

import jax
import jax.numpy as jnp
from jax import lax
from jax.experimental import pallas as pl
from jax.experimental.pallas import tpu as pltpu
from jax.sharding import PartitionSpec as P

MESH = pl.DeviceIdType.MESH
F32, BF16, I32 = jnp.float32, jnp.bfloat16, jnp.int32
DISTINCT = 24
SIDE = 8
LANES = 128
HOPS = (4, 3, 5, 2, 6, 1, 7, 0)
EARLY = 2
eps = 1e-06
exponential_sharpness = 0.025


def iota(shape, dim):
    return lax.broadcasted_iota(I32, shape, dim)


def total_of(ref, sem):
    return pltpu.make_async_copy(ref, ref, sem)


def kernel(n_row, n_col, ids_hbm, cnt_hbm, new_hbm, aux_hbm, emb_hbm, out_ref,
           ids_ref, cnt_ref, new_all, aux_tab, emb_tab, row_hot, lo_hot, ranks, lists, asked, sel,
           send_aux, send_emb, got_aux, got_emb, code_own, codes, slot_wide, w_wide, w_slots,
           met, gath, part, parts,
           tab_sem, list_send, list_recv, new_send, new_recv, code_send, code_recv, aux_send, aux_recv,
           emb_send, emb_recv, met_send, met_recv, part_send, part_recv):
    slots_row, new_dev = ids_ref.shape
    old_dev, width = aux_hbm.shape
    his = old_dev // LANES
    line = SIDE * DISTINCT
    me = lax.axis_index("row")
    my_col = lax.axis_index("col")
    core = lax.rem(my_col, 2)
    u_step = SIDE - (SIDE - 1) * core
    v_step = SIDE + 1 - u_step
    y, z = lax.div(me, SIDE), lax.rem(me, SIDE)
    u = y + (z - y) * core
    v = z + (y - z) * core

    def at_row(uu, vv):
        return {"row": uu * u_step + vv * v_step}

    def plus(a, d):
        return lax.rem(a + (d % SIDE), SIDE)

    loads = [pltpu.make_async_copy(ids_hbm, ids_ref, tab_sem.at[0]),
             pltpu.make_async_copy(cnt_hbm, cnt_ref, tab_sem.at[1]),
             pltpu.make_async_copy(new_hbm, new_all.at[u], tab_sem.at[2]),
             pltpu.make_async_copy(aux_hbm, aux_tab, tab_sem.at[3]),
             pltpu.make_async_copy(emb_hbm, emb_tab, tab_sem.at[4])]
    for t in loads:
        t.start()

    barrier = pltpu.get_barrier_semaphore()
    for dv in range(SIDE):
        for du in range(SIDE):
            if (du, dv) != (0, 0):
                pl.semaphore_signal(barrier, inc=1, device_id=at_row(plus(u, du), plus(v, dv)), device_id_type=MESH)
    for c in range(1, n_col):
        pl.semaphore_signal(barrier, inc=1, device_id={"col": lax.rem(my_col + c, n_col)}, device_id_type=MESH)

    loads[0].wait()
    loads[1].wait()
    ids = ids_ref[...]
    live = iota(ids.shape, 0) < cnt_ref[...]
    group = jnp.where(live, ids, 0) >> 7
    lo = ids & (LANES - 1)
    own = (group * 205) >> 11
    hi = group - his * own
    at = jnp.where(live, hi * n_row + own, -1)
    sub_all = iota((his * n_row, new_dev), 0)
    sub_lo = iota((LANES, new_dev), 0)
    for k in range(slots_row):
        cols = slice(k * new_dev, (k + 1) * new_dev)
        row_hot[:, cols] = jnp.where(sub_all == at[k:k + 1, :], 1.0, 0.0).astype(BF16)
        lo_hot[:, cols] = jnp.where(sub_lo == lo[k:k + 1, :], 1.0, 0.0).astype(BF16)
    named = lax.dot_general(row_hot[...], lo_hot[...], (((1,), (1,)), ((), ())), preferred_element_type=F32)
    present = named > 0.5
    mask = jnp.where(present, 1.0, 0.0).astype(BF16)
    i0, i1 = iota((LANES, LANES), 0), iota((LANES, LANES), 1)
    before = jnp.dot(mask, jnp.where(i0 < i1, 1.0, 0.0).astype(BF16), preferred_element_type=F32)
    per_row = jnp.dot(mask, jnp.ones((LANES, LANES), BF16), preferred_element_type=F32)
    ahead = jnp.zeros((n_row, LANES), F32)
    for h in range(his):
        rows = slice(h * n_row, (h + 1) * n_row)
        ranks[rows, :] = jnp.where(present[rows], before[rows] + ahead, -1.0)
        ahead = ahead + per_row[rows]

    lane = iota((n_row, LANES), 1)
    lane_f = lane.astype(F32)
    table = jnp.zeros((n_row, LANES), F32)
    for c in range(DISTINCT):
        acc = jnp.zeros((n_row, LANES), F32)
        for h in range(his):
            acc = acc + jnp.where(ranks[h * n_row:(h + 1) * n_row, :] == float(c), lane_f + float(h * LANES), 0.0)
        table = jnp.where(lane == c, jnp.sum(acc, axis=1, keepdims=True), table)
    for o in range(n_row):
        lists[o] = table[o:o + 1, :]

    pl.semaphore_wait(barrier, n_row - 1 + n_col - 1)

    for dv in HOPS:
        for du in range(SIDE):
            uu, vv = plus(u, -du), plus(v, -dv)
            mine = lists.at[uu * u_step + vv * v_step]
            if (du, dv) == (0, 0):
                pltpu.make_async_copy(mine, asked.at[0, u], list_recv.at[0]).start()
            else:
                pltpu.make_async_remote_copy(mine, asked.at[dv, u], list_send, list_recv.at[dv],
                                             device_id=at_row(uu, vv), device_id_type=MESH).start()

    loads[2].wait()
    for du in (4, 3, 5, 2, 6, 1, 7):
        pltpu.make_async_remote_copy(new_all.at[u], new_all.at[u], new_send, new_recv,
                                     device_id=at_row(plus(u, du), v), device_id_type=MESH).start()

    found = lax.dot_general(ranks[...].astype(BF16), row_hot[...], (((0,), (0,)), ((), ())), preferred_element_type=F32)
    own_y, own_z = own >> 3, own & (SIDE - 1)
    own_uv = (own_y + (own_z - own_y) * core) * SIDE + own_z + (own_y - own_z) * core
    for k in range(slots_row):
        cols = slice(k * new_dev, (k + 1) * new_dev)
        pos = jnp.sum(jnp.where(sub_lo == lo[k:k + 1, :], found[:, cols], 0.0), axis=0, keepdims=True)
        code_own[k:k + 1, :] = jnp.where(live[k:k + 1, :], own_uv[k:k + 1, :] * DISTINCT + pos.astype(I32), -1)
    pltpu.make_async_copy(code_own, codes.at[u], code_recv).start()
    for du in (4, 3, 5, 2, 6, 1, 7):
        pltpu.make_async_remote_copy(code_own, codes.at[u], code_send, code_recv,
                                     device_id=at_row(plus(u, du), v), device_id_type=MESH).start()

    loads[3].wait()
    loads[4].wait()

    wide = iota((DISTINCT, old_dev), 1).astype(F32)

    def gather(dv, tab, dst):
        rows = jnp.dot(sel[dv * line:(dv + 1) * line, :], tab[...], preferred_element_type=F32)
        for a in range(SIDE):
            dst[dv, a] = rows[a * DISTINCT:(a + 1) * DISTINCT].astype(BF16)

    for dv in HOPS:
        total_of(asked.at[dv], list_recv.at[dv]).wait()
        want = jnp.concatenate([asked[dv, a] for a in range(SIDE)], axis=0).T
        for a in range(0, SIDE, 2):
            pair = jnp.concatenate(
                [jnp.where(want[:DISTINCT, b:b + 1] == wide, 1.0, 0.0) for b in (a, a + 1)], axis=0)
            sel[dv * line + a * DISTINCT:dv * line + (a + 2) * DISTINCT, :] = pair.astype(BF16)
        gather(dv, aux_tab, send_aux)
        if dv == 0:
            pltpu.make_async_copy(send_aux.at[0], got_aux.at[v], aux_recv).start()
        else:
            pltpu.make_async_remote_copy(send_aux.at[dv], got_aux.at[v], aux_send, aux_recv,
                                         device_id=at_row(u, plus(v, dv)), device_id_type=MESH).start()
    for dv in HOPS:
        gather(dv, emb_tab, send_emb)

    def send_line(dv):
        for du in (4, 3, 5, 2, 6, 1, 7, 0):
            uu, vv = plus(u, du), plus(v, dv)
            if (du, dv) == (0, 0):
                pltpu.make_async_copy(send_emb.at[0, u], got_emb.at[u * SIDE + v], emb_recv).start()
            else:
                pltpu.make_async_remote_copy(send_emb.at[dv, uu], got_emb.at[u * SIDE + v], emb_send, emb_recv,
                                             device_id=at_row(uu, vv), device_id_type=MESH).start()

    total_of(send_aux.at[pl.ds(0, SIDE - 1)], aux_send).wait()
    for dv in HOPS[:EARLY]:
        send_line(dv)

    own_sq = jnp.sum(jnp.square(new_all[u].astype(F32)), axis=1, keepdims=True)
    part[2 * slots_row:2 * slots_row + 8, :] = jnp.broadcast_to(own_sq, (new_dev, LANES)).T[0:8, :]

    total_of(new_all.at[pl.ds(0, SIDE - 1)], new_recv).wait()
    total_of(codes, code_recv).wait()
    total_of(got_aux, aux_recv).wait()

    sub8 = iota((8, new_dev), 0)

    def meet(a, carry):
        new = new_all[a]
        acc = [jnp.zeros((8, new_dev), F32) for _ in range(2 * slots_row)]
        code = codes[a] - u * line
        rows = jnp.concatenate([got_aux[b, a] for b in range(SIDE)], axis=0)
        prod = lax.dot_general(rows, new, (((1,), (1,)), ((), ())), preferred_element_type=F32)
        near = jnp.broadcast_to(jnp.sum(jnp.square(rows.astype(F32)), axis=1, keepdims=True), (line, new_dev))
        for t in range(line // 8):
            here = sub8 + 8 * t
            for k in range(slots_row):
                hit = code[k:k + 1, :] == here
                acc[k] = acc[k] + jnp.where(hit, prod[8 * t:8 * t + 8], 0.0)
                acc[slots_row + k] = acc[slots_row + k] + jnp.where(hit, near[8 * t:8 * t + 8], 0.0)
        for k in range(2 * slots_row):
            met[a, k:k + 1, :] = jnp.sum(acc[k], axis=0, keepdims=True)
        return carry

    lax.fori_loop(0, SIDE, meet, 0)
    for du in (4, 3, 5, 2, 6, 1, 7, 0):
        uu = plus(u, du)
        if du == 0:
            pltpu.make_async_copy(met.at[u], gath.at[u], met_recv).start()
        else:
            pltpu.make_async_remote_copy(met.at[uu], gath.at[u], met_send, met_recv,
                                         device_id=at_row(uu, v), device_id_type=MESH).start()
    for dv in HOPS[EARLY:]:
        send_line(dv)

    for k in range(slots_row):
        slot_wide[k] = jnp.broadcast_to(code_own[k:k + 1, :], (8, new_dev))
    total_of(gath, met_recv).wait()
    both = gath[0]
    for a in range(1, SIDE):
        both = both + gath[a]
    part[0:2 * slots_row, :] = both
    for c in range(1, n_col):
        pltpu.make_async_remote_copy(part, parts.at[c - 1], part_send, part_recv,
                                     device_id={"col": lax.rem(my_col + c, n_col)}, device_id_type=MESH).start()
    total = part[...]
    total_of(parts, part_recv).wait()
    for c in range(1, n_col):
        total = total + parts[c - 1]

    inner, near_sq = total[:slots_row], total[slots_row:2 * slots_row]
    own_all = total[2 * slots_row:2 * slots_row + 1]
    similarity = inner * lax.rsqrt((own_all + eps) * (near_sq + eps))
    raw = jnp.where(live, jnp.exp(similarity / exponential_sharpness), 0.0)
    weights = (raw / jnp.sum(raw, axis=0, keepdims=True)).astype(BF16).astype(F32)
    for k in range(slots_row):
        w_wide[k] = jnp.broadcast_to(weights[k:k + 1, :], (8, new_dev))

    def weigh(o, c):
        for t in range(DISTINCT // 8):
            start = pl.multiple_of(o * DISTINCT + 8 * t, 8)
            here = sub8 + start
            acc = jnp.zeros((8, new_dev), F32)
            for k in range(slots_row):
                acc = acc + jnp.where(slot_wide[k] == here, w_wide[k], 0.0)
            w_slots[pl.ds(start, 8), :] = acc
        return c
    lax.fori_loop(0, n_row, weigh, 0)
    w_t = w_slots[...].T.astype(BF16)

    total_of(got_emb, emb_recv).wait()
    near_emb = got_emb[...].reshape(n_row * DISTINCT, width)
    out_ref[...] = jnp.dot(w_t, near_emb, preferred_element_type=F32).astype(BF16)

    total_of(lists.at[pl.ds(0, n_row - 1)], list_send).wait()
    total_of(new_all.at[pl.ds(0, SIDE - 1)], new_send).wait()
    total_of(codes.at[pl.ds(0, SIDE - 1)], code_send).wait()
    total_of(got_emb.at[pl.ds(0, n_row - 1)], emb_send).wait()
    total_of(met.at[pl.ds(0, SIDE - 1)], met_send).wait()
    total_of(parts, part_send).wait()


def solution(mesh):
    n_row, n_col = mesh.shape["row"], mesh.shape["col"]

    def local(new_aux, former_auxiliary_rows, old_emb, neighbour_ids, neighbour_counts):
        new_dev, width = new_aux.shape
        old_dev = former_auxiliary_rows.shape[0]
        slots_row = neighbour_ids.shape[1]
        slots = n_row * DISTINCT
        his = old_dev // LANES
        vm = pltpu.VMEM
        dma = pltpu.SemaphoreType.DMA
        hbm = pl.BlockSpec(memory_space=pl.ANY)
        return pl.pallas_call(
            functools.partial(kernel, n_row, n_col),
            out_shape=jax.ShapeDtypeStruct((new_dev, width), BF16),
            in_specs=[hbm] * 5,
            out_specs=pl.BlockSpec(memory_space=vm),
            scratch_shapes=[
                vm((slots_row, new_dev), I32), vm((1, new_dev), I32), vm((SIDE, new_dev, width), BF16),
                vm((old_dev, width), BF16), vm((old_dev, width), BF16),
                vm((his * n_row, slots_row * new_dev), BF16), vm((LANES, slots_row * new_dev), BF16),
                vm((his * n_row, LANES), F32), vm((n_row, 1, LANES), F32), vm((SIDE, SIDE, 1, LANES), F32),
                vm((slots, old_dev), BF16),
                vm((SIDE, SIDE, DISTINCT, width), BF16), vm((SIDE, SIDE, DISTINCT, width), BF16),
                vm((SIDE, SIDE, DISTINCT, width), BF16), vm((n_row, DISTINCT, width), BF16),
                vm((slots_row, new_dev), I32), vm((SIDE, slots_row, new_dev), I32),
                vm((slots_row, 8, new_dev), I32), vm((slots_row, 8, new_dev), F32),
                vm((slots, new_dev), F32),
                vm((SIDE, 2 * slots_row, new_dev), F32), vm((SIDE, 2 * slots_row, new_dev), F32),
                vm((2 * slots_row + 8, new_dev), F32), vm((n_col - 1, 2 * slots_row + 8, new_dev), F32),
                dma((5,)), dma(()), dma((SIDE,)), dma(()), dma(()), dma(()), dma(()), dma(()), dma(()),
                dma(()), dma(()), dma(()), dma(()), dma(()), dma(()),
            ],
            compiler_params=pltpu.CompilerParams(
                collective_id=0, has_side_effects=True, vmem_limit_bytes=67043328),
        )(neighbour_ids.T, neighbour_counts.reshape(1, new_dev), new_aux, former_auxiliary_rows, old_emb)

    return jax.shard_map(
        local,
        mesh=mesh,
        in_specs=(P("row", "col"), P("row", "col"), P("row", "col"), P("row", None), P("row")),
        out_specs=P("row", "col"),
        check_vma=False,
    )
```

```python
import functools

import jax
import jax.numpy as jnp
from jax import lax
from jax.experimental import pallas as pl
from jax.experimental.pallas import tpu as pltpu
from jax.sharding import PartitionSpec as P

MESH = pl.DeviceIdType.MESH
F32, BF16, I32 = jnp.float32, jnp.bfloat16, jnp.int32
DISTINCT = 24
SIDE = 8
LANES = 128
HOPS = (4, 3, 5, 2, 6, 1, 7, 0)
EARLY = 2
eps = 1e-06
exponential_sharpness = 0.025


def iota(shape, dim):
    return lax.broadcasted_iota(I32, shape, dim)


def total_of(ref, sem):
    return pltpu.make_async_copy(ref, ref, sem)


def kernel(n_row, n_col, ids_hbm, cnt_hbm, new_hbm, aux_hbm, emb_hbm, out_ref,
           ids_ref, cnt_ref, new_all, aux_tab, emb_tab, row_hot, lo_hot, ranks, lists, asked, sel,
           send_aux, send_emb, got_aux, got_emb, code_own, codes, slot_wide, w_wide, w_slots,
           met, gath, part, parts,
           tab_sem, list_send, list_recv, new_send, new_recv, code_send, code_recv, aux_send, aux_recv,
           emb_send, emb_recv, met_send, met_recv, part_send, part_recv):
    slots_row, new_dev = ids_ref.shape
    old_dev, width = aux_hbm.shape
    his = old_dev // LANES
    line = SIDE * DISTINCT
    me = lax.axis_index("row")
    my_col = lax.axis_index("col")
    core = lax.rem(my_col, 2)
    u_step = SIDE - (SIDE - 1) * core
    v_step = SIDE + 1 - u_step
    y, z = lax.div(me, SIDE), lax.rem(me, SIDE)
    u = y + (z - y) * core
    v = z + (y - z) * core

    def at_row(uu, vv):
        return {"row": uu * u_step + vv * v_step}

    def plus(a, d):
        return lax.rem(a + (d % SIDE), SIDE)

    loads = [pltpu.make_async_copy(ids_hbm, ids_ref, tab_sem.at[0]),
             pltpu.make_async_copy(cnt_hbm, cnt_ref, tab_sem.at[1]),
             pltpu.make_async_copy(new_hbm, new_all.at[u], tab_sem.at[2]),
             pltpu.make_async_copy(aux_hbm, aux_tab, tab_sem.at[3]),
             pltpu.make_async_copy(emb_hbm, emb_tab, tab_sem.at[4])]
    for t in loads:
        t.start()

    barrier = pltpu.get_barrier_semaphore()
    for dv in HOPS:
        for du in HOPS:
            if (du, dv) != (0, 0):
                pl.semaphore_signal(barrier, inc=1, device_id=at_row(plus(u, du), plus(v, dv)), device_id_type=MESH)
    for c in range(1, n_col):
        pl.semaphore_signal(barrier, inc=1, device_id={"col": lax.rem(my_col + c, n_col)}, device_id_type=MESH)

    loads[0].wait()
    loads[1].wait()
    ids = ids_ref[...]
    live = iota(ids.shape, 0) < cnt_ref[...]
    group = jnp.where(live, ids, 0) >> 7
    lo = ids & (LANES - 1)
    own = (group * 205) >> 11
    hi = group - his * own
    at = jnp.where(live, hi * n_row + own, -1)
    sub_all = iota((his * n_row, new_dev), 0)
    sub_lo = iota((LANES, new_dev), 0)
    for k in range(slots_row):
        cols = slice(k * new_dev, (k + 1) * new_dev)
        row_hot[:, cols] = jnp.where(sub_all == at[k:k + 1, :], 1.0, 0.0).astype(BF16)
        lo_hot[:, cols] = jnp.where(sub_lo == lo[k:k + 1, :], 1.0, 0.0).astype(BF16)
    named = lax.dot_general(row_hot[...], lo_hot[...], (((1,), (1,)), ((), ())), preferred_element_type=F32)
    present = named > 0.5
    mask = jnp.where(present, 1.0, 0.0).astype(BF16)
    i0, i1 = iota((LANES, LANES), 0), iota((LANES, LANES), 1)
    before = jnp.dot(mask, jnp.where(i0 < i1, 1.0, 0.0).astype(BF16), preferred_element_type=F32)
    per_row = jnp.dot(mask, jnp.ones((LANES, LANES), BF16), preferred_element_type=F32)
    ahead = jnp.zeros((n_row, LANES), F32)
    for h in range(his):
        rows = slice(h * n_row, (h + 1) * n_row)
        ranks[rows, :] = jnp.where(present[rows], before[rows] + ahead, -1.0)
        ahead = ahead + per_row[rows]

    lane = iota((n_row, LANES), 1)
    lane_f = lane.astype(F32)
    table = jnp.zeros((n_row, LANES), F32)
    for c in range(DISTINCT):
        acc = jnp.zeros((n_row, LANES), F32)
        for h in range(his):
            acc = acc + jnp.where(ranks[h * n_row:(h + 1) * n_row, :] == float(c), lane_f + float(h * LANES), 0.0)
        table = jnp.where(lane == c, jnp.sum(acc, axis=1, keepdims=True), table)
    for o in range(n_row):
        lists[o] = table[o:o + 1, :]

    pl.semaphore_wait(barrier, n_row - 1 + n_col - 1)

    for dv in HOPS:
        for du in HOPS:
            uu, vv = plus(u, -du), plus(v, -dv)
            mine = lists.at[uu * u_step + vv * v_step]
            if (du, dv) == (0, 0):
                pltpu.make_async_copy(mine, asked.at[0, u], list_recv.at[0]).start()
            else:
                pltpu.make_async_remote_copy(mine, asked.at[dv, u], list_send, list_recv.at[dv],
                                             device_id=at_row(uu, vv), device_id_type=MESH).start()

    def hand(block, du):
        src = new_all.at[plus(u, -block)]
        pltpu.make_async_remote_copy(src, src, new_send, new_recv.at[(block + du) % SIDE],
                                     device_id=at_row(plus(u, du), v), device_id_type=MESH).start()

    def block_in(block):
        total_of(new_all.at[plus(u, -block)], new_recv.at[block]).wait()

    loads[2].wait()
    for du in (2, 6, 1, 7):
        hand(0, du)

    found = lax.dot_general(ranks[...].astype(BF16), row_hot[...], (((0,), (0,)), ((), ())), preferred_element_type=F32)
    own_y, own_z = own >> 3, own & (SIDE - 1)
    own_u = own_y + (own_z - own_y) * core
    own_v = own_z + (own_y - own_z) * core
    nth = (3 * (u - own_u)) & (SIDE - 1)
    batch = (3 * (v - own_v - nth)) & (SIDE - 1)
    for k in range(slots_row):
        cols = slice(k * new_dev, (k + 1) * new_dev)
        pos = jnp.sum(jnp.where(sub_lo == lo[k:k + 1, :], found[:, cols], 0.0), axis=0, keepdims=True)
        pos = jnp.where(live[k:k + 1, :], pos.astype(I32), -n_row * DISTINCT)
        code_own[k:k + 1, :] = (own_u * SIDE + own_v)[k:k + 1, :] * DISTINCT + pos
        slot_wide[k] = jnp.broadcast_to((batch * SIDE + nth)[k:k + 1, :] * DISTINCT + pos, (8, new_dev))
    pltpu.make_async_copy(code_own, codes.at[u], code_recv).start()
    for du in (4, 3, 5, 2, 6, 1, 7):
        pltpu.make_async_remote_copy(code_own, codes.at[u], code_send, code_recv,
                                     device_id=at_row(plus(u, du), v), device_id_type=MESH).start()

    loads[3].wait()
    loads[4].wait()

    wide = iota((DISTINCT, old_dev), 1).astype(F32)

    def gather(dv, tab, dst):
        rows = jnp.dot(sel[dv * line:(dv + 1) * line, :], tab[...], preferred_element_type=F32)
        for a in range(SIDE):
            dst[dv, a] = rows[a * DISTINCT:(a + 1) * DISTINCT].astype(BF16)

    for dv in HOPS:
        total_of(asked.at[dv], list_recv.at[dv]).wait()
        want = jnp.concatenate([asked[dv, a] for a in range(SIDE)], axis=0).T
        for a in range(0, SIDE, 2):
            pair = jnp.concatenate(
                [jnp.where(want[:DISTINCT, b:b + 1] == wide, 1.0, 0.0) for b in (a, a + 1)], axis=0)
            sel[dv * line + a * DISTINCT:dv * line + (a + 2) * DISTINCT, :] = pair.astype(BF16)
        gather(dv, aux_tab, send_aux)
        if dv == 0:
            pltpu.make_async_copy(send_aux.at[0], got_aux.at[v], aux_recv).start()
        else:
            pltpu.make_async_remote_copy(send_aux.at[dv], got_aux.at[v], aux_send, aux_recv,
                                         device_id=at_row(u, plus(v, dv)), device_id_type=MESH).start()
    block_in(2)
    hand(2, 2)
    hand(2, 1)
    block_in(6)
    hand(6, 7)
    for dv in HOPS:
        gather(dv, emb_tab, send_emb)

    def send_line(q):
        for p in range(SIDE):
            du, dv = (3 * p) % SIDE, (3 * q + p) % SIDE
            uu, vv = plus(u, du), plus(v, dv)
            if (du, dv) == (0, 0):
                pltpu.make_async_copy(send_emb.at[0, u], got_emb.at[0], emb_recv.at[0]).start()
            else:
                pltpu.make_async_remote_copy(send_emb.at[dv, uu], got_emb.at[q * SIDE + p], emb_send, emb_recv.at[q],
                                             device_id=at_row(uu, vv), device_id_type=MESH).start()

    total_of(send_aux.at[pl.ds(0, SIDE - 1)], aux_send).wait()
    for q in range(EARLY):
        send_line(q)

    own_sq = jnp.sum(jnp.square(new_all[u].astype(F32)), axis=1, keepdims=True)
    part[2 * slots_row:2 * slots_row + 8, :] = jnp.broadcast_to(own_sq, (new_dev, LANES)).T[0:8, :]

    for block in (1, 7, 3, 5, 4):
        block_in(block)
    total_of(codes, code_recv).wait()
    total_of(got_aux, aux_recv).wait()

    sub8 = iota((8, new_dev), 0)

    def meet(a, carry):
        new = new_all[a]
        acc = [jnp.zeros((8, new_dev), F32) for _ in range(2 * slots_row)]
        code = codes[a] - u * line
        rows = jnp.concatenate([got_aux[b, a] for b in range(SIDE)], axis=0)
        prod = lax.dot_general(rows, new, (((1,), (1,)), ((), ())), preferred_element_type=F32)
        near = jnp.broadcast_to(jnp.sum(jnp.square(rows.astype(F32)), axis=1, keepdims=True), (line, new_dev))
        for t in range(line // 8):
            here = sub8 + 8 * t
            for k in range(slots_row):
                hit = code[k:k + 1, :] == here
                acc[k] = acc[k] + jnp.where(hit, prod[8 * t:8 * t + 8], 0.0)
                acc[slots_row + k] = acc[slots_row + k] + jnp.where(hit, near[8 * t:8 * t + 8], 0.0)
        for k in range(2 * slots_row):
            met[a, k:k + 1, :] = jnp.sum(acc[k], axis=0, keepdims=True)
        return carry

    lax.fori_loop(0, SIDE, meet, 0)
    for du in (4, 3, 5, 2, 6, 1, 7, 0):
        uu = plus(u, du)
        if du == 0:
            pltpu.make_async_copy(met.at[u], gath.at[u], met_recv).start()
        else:
            pltpu.make_async_remote_copy(met.at[uu], gath.at[u], met_send, met_recv,
                                         device_id=at_row(uu, v), device_id_type=MESH).start()
    for q in range(EARLY, SIDE):
        send_line(q)

    total_of(gath, met_recv).wait()
    both = gath[0]
    for a in range(1, SIDE):
        both = both + gath[a]
    part[0:2 * slots_row, :] = both
    for c in range(1, n_col):
        pltpu.make_async_remote_copy(part, parts.at[c - 1], part_send, part_recv,
                                     device_id={"col": lax.rem(my_col + c, n_col)}, device_id_type=MESH).start()
    total = part[...]
    total_of(parts, part_recv).wait()
    for c in range(1, n_col):
        total = total + parts[c - 1]

    inner, near_sq = total[:slots_row], total[slots_row:2 * slots_row]
    own_all = total[2 * slots_row:2 * slots_row + 1]
    similarity = inner * lax.rsqrt((own_all + eps) * (near_sq + eps))
    raw = jnp.where(live, jnp.exp(similarity / exponential_sharpness), 0.0)
    weights = (raw / jnp.sum(raw, axis=0, keepdims=True)).astype(BF16).astype(F32)
    for k in range(slots_row):
        w_wide[k] = jnp.broadcast_to(weights[k:k + 1, :], (8, new_dev))

    def weigh(o, c):
        for t in range(DISTINCT // 8):
            start = pl.multiple_of(o * DISTINCT + 8 * t, 8)
            here = sub8 + start
            acc = jnp.zeros((8, new_dev), F32)
            for k in range(slots_row):
                acc = acc + jnp.where(slot_wide[k] == here, w_wide[k], 0.0)
            w_slots[pl.ds(start, 8), :] = acc
        return c
    lax.fori_loop(0, n_row, weigh, 0)
    w_t = w_slots[...].T.astype(BF16)

    def blend(first, last):
        for q in range(first, last):
            total_of(got_emb.at[pl.ds(q * SIDE, SIDE)], emb_recv.at[q]).wait()
        rows = got_emb[first * SIDE:last * SIDE].reshape((last - first) * line, width)
        return jnp.dot(w_t[:, first * line:last * line], rows, preferred_element_type=F32)

    out_ref[...] = (blend(0, SIDE - 2) + blend(SIDE - 2, SIDE)).astype(BF16)

    total_of(lists.at[pl.ds(0, n_row - 1)], list_send).wait()
    total_of(new_all.at[pl.ds(0, SIDE - 1)], new_send).wait()
    total_of(codes.at[pl.ds(0, SIDE - 1)], code_send).wait()
    total_of(got_emb.at[pl.ds(0, n_row - 1)], emb_send).wait()
    total_of(met.at[pl.ds(0, SIDE - 1)], met_send).wait()
    total_of(parts, part_send).wait()


def solution(mesh):
    n_row, n_col = mesh.shape["row"], mesh.shape["col"]

    def local(new_aux, former_auxiliary_rows, old_emb, neighbour_ids, neighbour_counts):
        new_dev, width = new_aux.shape
        old_dev = former_auxiliary_rows.shape[0]
        slots_row = neighbour_ids.shape[1]
        slots = n_row * DISTINCT
        his = old_dev // LANES
        vm = pltpu.VMEM
        dma = pltpu.SemaphoreType.DMA
        hbm = pl.BlockSpec(memory_space=pl.ANY)
        return pl.pallas_call(
            functools.partial(kernel, n_row, n_col),
            out_shape=jax.ShapeDtypeStruct((new_dev, width), BF16),
            in_specs=[hbm] * 5,
            out_specs=pl.BlockSpec(memory_space=vm),
            scratch_shapes=[
                vm((slots_row, new_dev), I32), vm((1, new_dev), I32), vm((SIDE, new_dev, width), BF16),
                vm((old_dev, width), BF16), vm((old_dev, width), BF16),
                vm((his * n_row, slots_row * new_dev), BF16), vm((LANES, slots_row * new_dev), BF16),
                vm((his * n_row, LANES), F32), vm((n_row, 1, LANES), F32), vm((SIDE, SIDE, 1, LANES), F32),
                vm((slots, old_dev), BF16),
                vm((SIDE, SIDE, DISTINCT, width), BF16), vm((SIDE, SIDE, DISTINCT, width), BF16),
                vm((SIDE, SIDE, DISTINCT, width), BF16), vm((n_row, DISTINCT, width), BF16),
                vm((slots_row, new_dev), I32), vm((SIDE, slots_row, new_dev), I32),
                vm((slots_row, 8, new_dev), I32), vm((slots_row, 8, new_dev), F32),
                vm((slots, new_dev), F32),
                vm((SIDE, 2 * slots_row, new_dev), F32), vm((SIDE, 2 * slots_row, new_dev), F32),
                vm((2 * slots_row + 8, new_dev), F32), vm((n_col - 1, 2 * slots_row + 8, new_dev), F32),
                dma((5,)), dma(()), dma((SIDE,)), dma(()), dma((SIDE,)), dma(()), dma(()), dma(()), dma(()),
                dma(()), dma((SIDE,)), dma(()), dma(()), dma(()), dma(()),
            ],
            compiler_params=pltpu.CompilerParams(
                collective_id=0, has_side_effects=True, vmem_limit_bytes=67043328),
        )(neighbour_ids.T, neighbour_counts.reshape(1, new_dev), new_aux, former_auxiliary_rows, old_emb)

    return jax.shard_map(
        local,
        mesh=mesh,
        in_specs=(P("row", "col"), P("row", "col"), P("row", "col"), P("row", None), P("row")),
        out_specs=P("row", "col"),
        check_vma=False,
    )
```

```python
import functools

import jax
import jax.numpy as jnp
from jax import lax
from jax.experimental import pallas as pl
from jax.experimental.pallas import tpu as pltpu
from jax.sharding import PartitionSpec as P

MESH = pl.DeviceIdType.MESH
F32, BF16, I32 = jnp.float32, jnp.bfloat16, jnp.int32
DISTINCT = 24
SIDE = 8
LANES = 128
HOPS = (4, 3, 5, 2, 6, 1, 7, 0)
EARLY = 2
LATE = 5
eps = 1e-06
exponential_sharpness = 0.025


def iota(shape, dim):
    return lax.broadcasted_iota(I32, shape, dim)


def total_of(ref, sem):
    return pltpu.make_async_copy(ref, ref, sem)


def kernel(n_row, n_col, ids_hbm, cnt_hbm, new_hbm, aux_hbm, emb_hbm, out_ref,
           ids_ref, cnt_ref, new_all, aux_tab, emb_tab, row_hot, lo_hot, ranks, lists, asked, sel,
           send_aux, send_emb, got_aux, got_emb, code_own, codes, slot_wide, w_wide, w_slots,
           met, gath, part, parts,
           tab_sem, list_send, list_recv, new_send, new_recv, code_send, code_recv, aux_send, aux_recv,
           emb_send, emb_recv, met_send, met_recv, part_send, part_recv):
    slots_row, new_dev = ids_ref.shape
    old_dev, width = aux_hbm.shape
    his = old_dev // LANES
    line = SIDE * DISTINCT
    me = lax.axis_index("row")
    my_col = lax.axis_index("col")
    core = lax.rem(my_col, 2)
    u_step = SIDE - (SIDE - 1) * core
    v_step = SIDE + 1 - u_step
    y, z = lax.div(me, SIDE), lax.rem(me, SIDE)
    u = y + (z - y) * core
    v = z + (y - z) * core

    def at_row(uu, vv):
        return {"row": uu * u_step + vv * v_step}

    def plus(a, d):
        return lax.rem(a + (d % SIDE), SIDE)

    loads = [pltpu.make_async_copy(ids_hbm, ids_ref, tab_sem.at[0]),
             pltpu.make_async_copy(cnt_hbm, cnt_ref, tab_sem.at[1]),
             pltpu.make_async_copy(new_hbm, new_all.at[u], tab_sem.at[2]),
             pltpu.make_async_copy(aux_hbm, aux_tab, tab_sem.at[3]),
             pltpu.make_async_copy(emb_hbm, emb_tab, tab_sem.at[4])]
    for t in loads:
        t.start()

    barrier = pltpu.get_barrier_semaphore()
    for dv in HOPS:
        for du in HOPS:
            if (du, dv) != (0, 0):
                pl.semaphore_signal(barrier, inc=1, device_id=at_row(plus(u, du), plus(v, dv)), device_id_type=MESH)
    for c in range(1, n_col):
        pl.semaphore_signal(barrier, inc=1, device_id={"col": lax.rem(my_col + c, n_col)}, device_id_type=MESH)

    loads[0].wait()
    loads[1].wait()
    ids = ids_ref[...]
    live = iota(ids.shape, 0) < cnt_ref[...]
    group = jnp.where(live, ids, 0) >> 7
    lo = ids & (LANES - 1)
    own = (group * 205) >> 11
    hi = group - his * own
    at = jnp.where(live, hi * n_row + own, -1)
    sub_all = iota((his * n_row, new_dev), 0)
    sub_lo = iota((LANES, new_dev), 0)
    for k in range(slots_row):
        cols = slice(k * new_dev, (k + 1) * new_dev)
        row_hot[:, cols] = jnp.where(sub_all == at[k:k + 1, :], 1.0, 0.0).astype(BF16)
        lo_hot[:, cols] = jnp.where(sub_lo == lo[k:k + 1, :], 1.0, 0.0).astype(BF16)
    named = lax.dot_general(row_hot[...], lo_hot[...], (((1,), (1,)), ((), ())), preferred_element_type=F32)
    present = named > 0.5
    mask = jnp.where(present, 1.0, 0.0).astype(BF16)
    i0, i1 = iota((LANES, LANES), 0), iota((LANES, LANES), 1)
    before = jnp.dot(mask, jnp.where(i0 < i1, 1.0, 0.0).astype(BF16), preferred_element_type=F32)
    per_row = jnp.dot(mask, jnp.ones((LANES, LANES), BF16), preferred_element_type=F32)
    ahead = jnp.zeros((n_row, LANES), F32)
    for h in range(his):
        rows = slice(h * n_row, (h + 1) * n_row)
        ranks[rows, :] = jnp.where(present[rows], before[rows] + ahead, -1.0)
        ahead = ahead + per_row[rows]

    lane = iota((n_row, LANES), 1)
    lane_f = lane.astype(F32)
    table = jnp.zeros((n_row, LANES), F32)
    for c in range(DISTINCT):
        acc = jnp.zeros((n_row, LANES), F32)
        for h in range(his):
            acc = acc + jnp.where(ranks[h * n_row:(h + 1) * n_row, :] == float(c), lane_f + float(h * LANES), 0.0)
        table = jnp.where(lane == c, jnp.sum(acc, axis=1, keepdims=True), table)
    for o in range(n_row):
        lists[o] = table[o:o + 1, :]

    pl.semaphore_wait(barrier, n_row - 1 + n_col - 1)

    for dv in HOPS:
        for du in HOPS:
            uu, vv = plus(u, -du), plus(v, -dv)
            mine = lists.at[uu * u_step + vv * v_step]
            if (du, dv) == (0, 0):
                pltpu.make_async_copy(mine, asked.at[0, u], list_recv.at[0]).start()
            else:
                pltpu.make_async_remote_copy(mine, asked.at[dv, u], list_send, list_recv.at[dv],
                                             device_id=at_row(uu, vv), device_id_type=MESH).start()

    def hand(block, du):
        src = new_all.at[plus(u, -block)]
        pltpu.make_async_remote_copy(src, src, new_send, new_recv.at[(block + du) % SIDE],
                                     device_id=at_row(plus(u, du), v), device_id_type=MESH).start()

    def block_in(block):
        total_of(new_all.at[plus(u, -block)], new_recv.at[block]).wait()

    loads[2].wait()
    hand(0, 1)
    hand(0, 7)

    found = lax.dot_general(ranks[...].astype(BF16), row_hot[...], (((0,), (0,)), ((), ())), preferred_element_type=F32)
    own_y, own_z = own >> 3, own & (SIDE - 1)
    own_u = own_y + (own_z - own_y) * core
    own_v = own_z + (own_y - own_z) * core

    def place_of(d):
        far = (d & (SIDE - 1)) - SIDE // 2
        return jnp.where(far > 0, 2 * far, jnp.where(far < 0, -2 * far - 1, 0))

    nth = place_of(u - own_u)
    batch = place_of(v - own_v - 3 * (u - own_u))
    for k in range(slots_row):
        cols = slice(k * new_dev, (k + 1) * new_dev)
        pos = jnp.sum(jnp.where(sub_lo == lo[k:k + 1, :], found[:, cols], 0.0), axis=0, keepdims=True)
        pos = jnp.where(live[k:k + 1, :], pos.astype(I32), -n_row * DISTINCT)
        code_own[k:k + 1, :] = (own_u * SIDE + own_v)[k:k + 1, :] * DISTINCT + pos
        slot_wide[k] = jnp.broadcast_to((batch * SIDE + nth)[k:k + 1, :] * DISTINCT + pos, (8, new_dev))
    pltpu.make_async_copy(code_own, codes.at[u], code_recv).start()
    for du in (4, 3, 5, 2, 6, 1, 7):
        pltpu.make_async_remote_copy(code_own, codes.at[u], code_send, code_recv,
                                     device_id=at_row(plus(u, du), v), device_id_type=MESH).start()

    block_in(1)
    hand(1, 1)
    block_in(7)
    hand(7, 7)

    loads[3].wait()
    loads[4].wait()

    wide = iota((DISTINCT, old_dev), 1).astype(F32)

    def gather(dv, tab, dst):
        rows = jnp.dot(sel[dv * line:(dv + 1) * line, :], tab[...], preferred_element_type=F32)
        for a in range(SIDE):
            dst[dv, a] = rows[a * DISTINCT:(a + 1) * DISTINCT].astype(BF16)

    for dv in HOPS:
        total_of(asked.at[dv], list_recv.at[dv]).wait()
        want = jnp.concatenate([asked[dv, a] for a in range(SIDE)], axis=0).T
        for a in range(0, SIDE, 2):
            pair = jnp.concatenate(
                [jnp.where(want[:DISTINCT, b:b + 1] == wide, 1.0, 0.0) for b in (a, a + 1)], axis=0)
            sel[dv * line + a * DISTINCT:dv * line + (a + 2) * DISTINCT, :] = pair.astype(BF16)
        gather(dv, aux_tab, send_aux)
        if dv == 0:
            pltpu.make_async_copy(send_aux.at[0], got_aux.at[v], aux_recv).start()
        else:
            pltpu.make_async_remote_copy(send_aux.at[dv], got_aux.at[v], aux_send, aux_recv,
                                         device_id=at_row(u, plus(v, dv)), device_id_type=MESH).start()
    block_in(2)
    hand(2, 1)
    block_in(6)
    hand(6, 7)
    for dv in HOPS:
        gather(dv, emb_tab, send_emb)
    block_in(3)
    hand(3, 1)

    def send_line(q):
        for p in range(SIDE):
            du = HOPS[p]
            dv = (3 * du + HOPS[q]) % SIDE
            uu, vv = plus(u, du), plus(v, dv)
            if (du, dv) == (0, 0):
                pltpu.make_async_copy(send_emb.at[0, u], got_emb.at[q * SIDE + p], emb_recv.at[q]).start()
            else:
                pltpu.make_async_remote_copy(send_emb.at[dv, uu], got_emb.at[q * SIDE + p], emb_send, emb_recv.at[q],
                                             device_id=at_row(uu, vv), device_id_type=MESH).start()


    own_sq = jnp.sum(jnp.square(new_all[u].astype(F32)), axis=1, keepdims=True)
    part[2 * slots_row:2 * slots_row + 8, :] = jnp.broadcast_to(own_sq, (new_dev, LANES)).T[0:8, :]

    block_in(5)
    block_in(4)
    total_of(codes, code_recv).wait()
    total_of(got_aux, aux_recv).wait()
    for q in range(EARLY):
        send_line(q)

    sub8 = iota((8, new_dev), 0)

    def meet(a, carry):
        new = new_all[a]
        acc = [jnp.zeros((8, new_dev), F32) for _ in range(2 * slots_row)]
        code = codes[a] - u * line
        rows = jnp.concatenate([got_aux[b, a] for b in range(SIDE)], axis=0)
        prod = lax.dot_general(rows, new, (((1,), (1,)), ((), ())), preferred_element_type=F32)
        near = jnp.broadcast_to(jnp.sum(jnp.square(rows.astype(F32)), axis=1, keepdims=True), (line, new_dev))
        for t in range(line // 8):
            here = sub8 + 8 * t
            for k in range(slots_row):
                hit = code[k:k + 1, :] == here
                acc[k] = acc[k] + jnp.where(hit, prod[8 * t:8 * t + 8], 0.0)
                acc[slots_row + k] = acc[slots_row + k] + jnp.where(hit, near[8 * t:8 * t + 8], 0.0)
        for k in range(2 * slots_row):
            met[a, k:k + 1, :] = jnp.sum(acc[k], axis=0, keepdims=True)
        return carry

    lax.fori_loop(0, SIDE, meet, 0)
    for du in (4, 3, 5, 2, 6, 1, 7, 0):
        uu = plus(u, du)
        if du == 0:
            pltpu.make_async_copy(met.at[u], gath.at[u], met_recv).start()
        else:
            pltpu.make_async_remote_copy(met.at[uu], gath.at[u], met_send, met_recv,
                                         device_id=at_row(uu, v), device_id_type=MESH).start()
    for q in range(EARLY, LATE):
        send_line(q)

    total_of(gath, met_recv).wait()
    for q in range(LATE, SIDE):
        send_line(q)
    both = gath[0]
    for a in range(1, SIDE):
        both = both + gath[a]
    part[0:2 * slots_row, :] = both
    for c in range(1, n_col):
        pltpu.make_async_remote_copy(part, parts.at[c - 1], part_send, part_recv,
                                     device_id={"col": lax.rem(my_col + c, n_col)}, device_id_type=MESH).start()
    total = part[...]
    total_of(parts, part_recv).wait()
    for c in range(1, n_col):
        total = total + parts[c - 1]

    inner, near_sq = total[:slots_row], total[slots_row:2 * slots_row]
    own_all = total[2 * slots_row:2 * slots_row + 1]
    similarity = inner * lax.rsqrt((own_all + eps) * (near_sq + eps))
    raw = jnp.where(live, jnp.exp(similarity / exponential_sharpness), 0.0)
    weights = (raw / jnp.sum(raw, axis=0, keepdims=True)).astype(BF16).astype(F32)
    for k in range(slots_row):
        w_wide[k] = jnp.broadcast_to(weights[k:k + 1, :], (8, new_dev))

    def weigh(o, c):
        for t in range(DISTINCT // 8):
            start = pl.multiple_of(o * DISTINCT + 8 * t, 8)
            here = sub8 + start
            acc = jnp.zeros((8, new_dev), F32)
            for k in range(slots_row):
                acc = acc + jnp.where(slot_wide[k] == here, w_wide[k], 0.0)
            w_slots[pl.ds(start, 8), :] = acc
        return c
    lax.fori_loop(0, n_row, weigh, 0)
    w_t = w_slots[...].T.astype(BF16)

    def blend(first, last):
        for q in range(first, last):
            total_of(got_emb.at[pl.ds(q * SIDE, SIDE)], emb_recv.at[q]).wait()
        rows = got_emb[first * SIDE:last * SIDE].reshape((last - first) * line, width)
        return jnp.dot(w_t[:, first * line:last * line], rows, preferred_element_type=F32)

    out_ref[...] = (blend(0, SIDE - 2) + blend(SIDE - 2, SIDE)).astype(BF16)

    total_of(lists.at[pl.ds(0, n_row - 1)], list_send).wait()
    total_of(send_aux.at[pl.ds(0, SIDE - 1)], aux_send).wait()
    total_of(new_all.at[pl.ds(0, SIDE - 1)], new_send).wait()
    total_of(codes.at[pl.ds(0, SIDE - 1)], code_send).wait()
    total_of(got_emb.at[pl.ds(0, n_row - 1)], emb_send).wait()
    total_of(met.at[pl.ds(0, SIDE - 1)], met_send).wait()
    total_of(parts, part_send).wait()


def solution(mesh):
    n_row, n_col = mesh.shape["row"], mesh.shape["col"]

    def local(new_aux, former_auxiliary_rows, old_emb, neighbour_ids, neighbour_counts):
        new_dev, width = new_aux.shape
        old_dev = former_auxiliary_rows.shape[0]
        slots_row = neighbour_ids.shape[1]
        slots = n_row * DISTINCT
        his = old_dev // LANES
        vm = pltpu.VMEM
        dma = pltpu.SemaphoreType.DMA
        hbm = pl.BlockSpec(memory_space=pl.ANY)
        return pl.pallas_call(
            functools.partial(kernel, n_row, n_col),
            out_shape=jax.ShapeDtypeStruct((new_dev, width), BF16),
            in_specs=[hbm] * 5,
            out_specs=pl.BlockSpec(memory_space=vm),
            scratch_shapes=[
                vm((slots_row, new_dev), I32), vm((1, new_dev), I32), vm((SIDE, new_dev, width), BF16),
                vm((old_dev, width), BF16), vm((old_dev, width), BF16),
                vm((his * n_row, slots_row * new_dev), BF16), vm((LANES, slots_row * new_dev), BF16),
                vm((his * n_row, LANES), F32), vm((n_row, 1, LANES), F32), vm((SIDE, SIDE, 1, LANES), F32),
                vm((slots, old_dev), BF16),
                vm((SIDE, SIDE, DISTINCT, width), BF16), vm((SIDE, SIDE, DISTINCT, width), BF16),
                vm((SIDE, SIDE, DISTINCT, width), BF16), vm((n_row, DISTINCT, width), BF16),
                vm((slots_row, new_dev), I32), vm((SIDE, slots_row, new_dev), I32),
                vm((slots_row, 8, new_dev), I32), vm((slots_row, 8, new_dev), F32),
                vm((slots, new_dev), F32),
                vm((SIDE, 2 * slots_row, new_dev), F32), vm((SIDE, 2 * slots_row, new_dev), F32),
                vm((2 * slots_row + 8, new_dev), F32), vm((n_col - 1, 2 * slots_row + 8, new_dev), F32),
                dma((5,)), dma(()), dma((SIDE,)), dma(()), dma((SIDE,)), dma(()), dma(()), dma(()), dma(()),
                dma(()), dma((SIDE,)), dma(()), dma(()), dma(()), dma(()),
            ],
            compiler_params=pltpu.CompilerParams(
                collective_id=0, has_side_effects=True, vmem_limit_bytes=67043328),
        )(neighbour_ids.T, neighbour_counts.reshape(1, new_dev), new_aux, former_auxiliary_rows, old_emb)

    return jax.shard_map(
        local,
        mesh=mesh,
        in_specs=(P("row", "col"), P("row", "col"), P("row", "col"), P("row", None), P("row")),
        out_specs=P("row", "col"),
        check_vma=False,
    )
```

```python
import functools

import jax
import jax.numpy as jnp
from jax import lax
from jax.experimental import pallas as pl
from jax.experimental.pallas import tpu as pltpu
from jax.sharding import PartitionSpec as P

MESH = pl.DeviceIdType.MESH
F32, BF16, I32 = jnp.float32, jnp.bfloat16, jnp.int32
DISTINCT = 24
SIDE = 8
LANES = 128
HOPS = (4, 3, 5, 2, 6, 1, 7, 0)
EARLY = 2
LATE = 5
eps = 1e-06
exponential_sharpness = 0.025


def iota(shape, dim):
    return lax.broadcasted_iota(I32, shape, dim)


def total_of(ref, sem):
    return pltpu.make_async_copy(ref, ref, sem)


def kernel(n_row, n_col, ids_hbm, cnt_hbm, new_hbm, aux_hbm, emb_hbm, out_ref,
           ids_ref, cnt_ref, new_all, aux_tab, emb_tab, row_hot, lo_hot, ranks, lists, asked, sel,
           send_aux, send_emb, got_aux, got_emb, code_own, codes, slot_wide, w_wide, w_slots,
           met, gath, part, parts,
           tab_sem, list_send, list_recv, new_send, new_recv, code_send, code_recv, aux_send, aux_recv,
           emb_send, emb_recv, met_send, met_recv, part_send, part_recv):
    slots_row, new_dev = ids_ref.shape
    old_dev, width = aux_hbm.shape
    his = old_dev // LANES
    line = SIDE * DISTINCT
    me = lax.axis_index("row")
    my_col = lax.axis_index("col")
    core = lax.rem(my_col, 2)
    u_step = SIDE - (SIDE - 1) * core
    v_step = SIDE + 1 - u_step
    y, z = lax.div(me, SIDE), lax.rem(me, SIDE)
    u = y + (z - y) * core
    v = z + (y - z) * core

    def at_row(uu, vv):
        return {"row": uu * u_step + vv * v_step}

    def plus(a, d):
        return lax.rem(a + (d % SIDE), SIDE)

    loads = [pltpu.make_async_copy(ids_hbm, ids_ref, tab_sem.at[0]),
             pltpu.make_async_copy(cnt_hbm, cnt_ref, tab_sem.at[1]),
             pltpu.make_async_copy(new_hbm, new_all.at[u], tab_sem.at[2]),
             pltpu.make_async_copy(aux_hbm, aux_tab, tab_sem.at[3]),
             pltpu.make_async_copy(emb_hbm, emb_tab, tab_sem.at[4])]
    for t in loads:
        t.start()

    barrier = pltpu.get_barrier_semaphore()
    for dv in HOPS:
        for du in HOPS:
            if (du, dv) != (0, 0):
                pl.semaphore_signal(barrier, inc=1, device_id=at_row(plus(u, du), plus(v, dv)), device_id_type=MESH)
    for c in range(1, n_col):
        pl.semaphore_signal(barrier, inc=1, device_id={"col": lax.rem(my_col + c, n_col)}, device_id_type=MESH)

    loads[0].wait()
    loads[1].wait()
    ids = ids_ref[...]
    live = iota(ids.shape, 0) < cnt_ref[...]
    group = jnp.where(live, ids, 0) >> 7
    lo = ids & (LANES - 1)
    own = (group * 205) >> 11
    hi = group - his * own
    at = jnp.where(live, hi * n_row + own, -1)
    sub_all = iota((his * n_row, new_dev), 0)
    sub_lo = iota((LANES, new_dev), 0)
    for k in range(slots_row):
        cols = slice(k * new_dev, (k + 1) * new_dev)
        row_hot[:, cols] = jnp.where(sub_all == at[k:k + 1, :], 1.0, 0.0).astype(BF16)
        lo_hot[:, cols] = jnp.where(sub_lo == lo[k:k + 1, :], 1.0, 0.0).astype(BF16)
    named = lax.dot_general(row_hot[...], lo_hot[...], (((1,), (1,)), ((), ())), preferred_element_type=F32)
    present = named > 0.5
    mask = jnp.where(present, 1.0, 0.0).astype(BF16)
    i0, i1 = iota((LANES, LANES), 0), iota((LANES, LANES), 1)
    before = jnp.dot(mask, jnp.where(i0 < i1, 1.0, 0.0).astype(BF16), preferred_element_type=F32)
    per_row = jnp.dot(mask, jnp.ones((LANES, LANES), BF16), preferred_element_type=F32)
    ahead = jnp.zeros((n_row, LANES), F32)
    for h in range(his):
        rows = slice(h * n_row, (h + 1) * n_row)
        ranks[rows, :] = jnp.where(present[rows], before[rows] + ahead, -1.0)
        ahead = ahead + per_row[rows]

    lane = iota((n_row, LANES), 1)
    lane_f = lane.astype(F32)
    table = jnp.zeros((n_row, LANES), F32)
    for c in range(DISTINCT):
        acc = jnp.zeros((n_row, LANES), F32)
        for h in range(his):
            acc = acc + jnp.where(ranks[h * n_row:(h + 1) * n_row, :] == float(c), lane_f + float(h * LANES), 0.0)
        table = jnp.where(lane == c, jnp.sum(acc, axis=1, keepdims=True), table)
    for o in range(n_row):
        lists[o] = table[o:o + 1, :]

    pl.semaphore_wait(barrier, n_row - 1 + n_col - 1)

    for dv in HOPS:
        for du in HOPS:
            uu, vv = plus(u, -du), plus(v, -dv)
            mine = lists.at[uu * u_step + vv * v_step]
            if (du, dv) == (0, 0):
                pltpu.make_async_copy(mine, asked.at[0, u], list_recv.at[0]).start()
            else:
                pltpu.make_async_remote_copy(mine, asked.at[dv, u], list_send, list_recv.at[dv],
                                             device_id=at_row(uu, vv), device_id_type=MESH).start()

    def hand(block, du):
        src = new_all.at[plus(u, -block)]
        pltpu.make_async_remote_copy(src, src, new_send, new_recv.at[(block + du) % SIDE],
                                     device_id=at_row(plus(u, du), v), device_id_type=MESH).start()

    def block_in(block):
        total_of(new_all.at[plus(u, -block)], new_recv.at[block]).wait()

    loads[2].wait()
    hand(0, 1)
    hand(0, 7)

    found = lax.dot_general(ranks[...].astype(BF16), row_hot[...], (((0,), (0,)), ((), ())), preferred_element_type=F32)
    own_y, own_z = own >> 3, own & (SIDE - 1)
    own_u = own_y + (own_z - own_y) * core
    own_v = own_z + (own_y - own_z) * core

    def place_of(d):
        far = (d & (SIDE - 1)) - SIDE // 2
        return jnp.where(far > 0, 2 * far, jnp.where(far < 0, -2 * far - 1, 0))

    nth = place_of(u - own_u)
    batch = place_of(v - own_v - 3 * (u - own_u))
    for k in range(slots_row):
        cols = slice(k * new_dev, (k + 1) * new_dev)
        pos = jnp.sum(jnp.where(sub_lo == lo[k:k + 1, :], found[:, cols], 0.0), axis=0, keepdims=True)
        pos = jnp.where(live[k:k + 1, :], pos.astype(I32), -n_row * DISTINCT)
        code_own[k:k + 1, :] = (own_u * SIDE + own_v)[k:k + 1, :] * DISTINCT + pos
        slot_wide[k] = jnp.broadcast_to((batch * SIDE + nth)[k:k + 1, :] * DISTINCT + pos, (8, new_dev))
    pltpu.make_async_copy(code_own, codes.at[u], code_recv).start()
    for du in (4, 3, 5, 2, 6, 1, 7):
        pltpu.make_async_remote_copy(code_own, codes.at[u], code_send, code_recv,
                                     device_id=at_row(plus(u, du), v), device_id_type=MESH).start()

    block_in(1)
    hand(1, 1)
    block_in(7)
    hand(7, 7)

    loads[3].wait()
    loads[4].wait()

    wide = iota((DISTINCT, old_dev), 1).astype(F32)

    def gather(dv, tab, dst):
        rows = jnp.dot(sel[dv * line:(dv + 1) * line, :], tab[...], preferred_element_type=F32)
        for a in range(SIDE):
            dst[dv, a] = rows[a * DISTINCT:(a + 1) * DISTINCT].astype(BF16)

    for dv in HOPS:
        total_of(asked.at[dv], list_recv.at[dv]).wait()
        want = jnp.concatenate([asked[dv, a] for a in range(SIDE)], axis=0).T
        for a in range(0, SIDE, 2):
            pair = jnp.concatenate(
                [jnp.where(want[:DISTINCT, b:b + 1] == wide, 1.0, 0.0) for b in (a, a + 1)], axis=0)
            sel[dv * line + a * DISTINCT:dv * line + (a + 2) * DISTINCT, :] = pair.astype(BF16)
        gather(dv, aux_tab, send_aux)
        if dv == 0:
            pltpu.make_async_copy(send_aux.at[0], got_aux.at[v], aux_recv).start()
        else:
            pltpu.make_async_remote_copy(send_aux.at[dv], got_aux.at[v], aux_send, aux_recv,
                                         device_id=at_row(u, plus(v, dv)), device_id_type=MESH).start()
    block_in(2)
    hand(2, 1)
    block_in(6)
    hand(6, 7)
    for dv in HOPS[:4]:
        gather(dv, emb_tab, send_emb)
    block_in(3)
    hand(3, 1)
    for dv in HOPS[4:]:
        gather(dv, emb_tab, send_emb)

    def send_line(q):
        for p in range(SIDE):
            du = HOPS[p]
            dv = (3 * du + HOPS[q]) % SIDE
            uu, vv = plus(u, du), plus(v, dv)
            if (du, dv) == (0, 0):
                pltpu.make_async_copy(send_emb.at[0, u], got_emb.at[q * SIDE + p], emb_recv.at[q]).start()
            else:
                pltpu.make_async_remote_copy(send_emb.at[dv, uu], got_emb.at[q * SIDE + p], emb_send, emb_recv.at[q],
                                             device_id=at_row(uu, vv), device_id_type=MESH).start()


    own_sq = jnp.sum(jnp.square(new_all[u].astype(F32)), axis=1, keepdims=True)
    part[2 * slots_row:2 * slots_row + 8, :] = jnp.broadcast_to(own_sq, (new_dev, LANES)).T[0:8, :]

    block_in(5)
    block_in(4)
    total_of(codes, code_recv).wait()
    total_of(got_aux, aux_recv).wait()
    for q in range(EARLY):
        send_line(q)

    sub8 = iota((8, new_dev), 0)

    def meet(a, carry):
        new = new_all[a]
        acc = [jnp.zeros((8, new_dev), F32) for _ in range(2 * slots_row)]
        code = codes[a] - u * line
        rows = jnp.concatenate([got_aux[b, a] for b in range(SIDE)], axis=0)
        prod = lax.dot_general(rows, new, (((1,), (1,)), ((), ())), preferred_element_type=F32)
        near = jnp.broadcast_to(jnp.sum(jnp.square(rows.astype(F32)), axis=1, keepdims=True), (line, new_dev))
        for t in range(line // 8):
            here = sub8 + 8 * t
            for k in range(slots_row):
                hit = code[k:k + 1, :] == here
                acc[k] = acc[k] + jnp.where(hit, prod[8 * t:8 * t + 8], 0.0)
                acc[slots_row + k] = acc[slots_row + k] + jnp.where(hit, near[8 * t:8 * t + 8], 0.0)
        for k in range(2 * slots_row):
            met[a, k:k + 1, :] = jnp.sum(acc[k], axis=0, keepdims=True)
        return carry

    lax.fori_loop(0, SIDE, meet, 0)
    for du in (4, 3, 5, 2, 6, 1, 7, 0):
        uu = plus(u, du)
        if du == 0:
            pltpu.make_async_copy(met.at[u], gath.at[u], met_recv).start()
        else:
            pltpu.make_async_remote_copy(met.at[uu], gath.at[u], met_send, met_recv,
                                         device_id=at_row(uu, v), device_id_type=MESH).start()
    for q in range(EARLY, LATE):
        send_line(q)

    total_of(gath, met_recv).wait()
    for q in range(LATE, SIDE):
        send_line(q)
    both = gath[0]
    for a in range(1, SIDE):
        both = both + gath[a]
    part[0:2 * slots_row, :] = both
    for c in range(1, n_col):
        pltpu.make_async_remote_copy(part, parts.at[c - 1], part_send, part_recv,
                                     device_id={"col": lax.rem(my_col + c, n_col)}, device_id_type=MESH).start()
    total = part[...]
    total_of(parts, part_recv).wait()
    for c in range(1, n_col):
        total = total + parts[c - 1]

    inner, near_sq = total[:slots_row], total[slots_row:2 * slots_row]
    own_all = total[2 * slots_row:2 * slots_row + 1]
    similarity = inner * lax.rsqrt((own_all + eps) * (near_sq + eps))
    raw = jnp.where(live, jnp.exp(similarity / exponential_sharpness), 0.0)
    weights = (raw / jnp.sum(raw, axis=0, keepdims=True)).astype(BF16).astype(F32)
    for k in range(slots_row):
        w_wide[k] = jnp.broadcast_to(weights[k:k + 1, :], (8, new_dev))

    def weigh(o, c):
        for t in range(DISTINCT // 8):
            start = pl.multiple_of(o * DISTINCT + 8 * t, 8)
            here = sub8 + start
            acc = jnp.zeros((8, new_dev), F32)
            for k in range(slots_row):
                acc = acc + jnp.where(slot_wide[k] == here, w_wide[k], 0.0)
            w_slots[pl.ds(start, 8), :] = acc
        return c
    lax.fori_loop(0, n_row, weigh, 0)
    w_t = w_slots[...].T.astype(BF16)

    def blend(first, last):
        for q in range(first, last):
            total_of(got_emb.at[pl.ds(q * SIDE, SIDE)], emb_recv.at[q]).wait()
        rows = got_emb[first * SIDE:last * SIDE].reshape((last - first) * line, width)
        return jnp.dot(w_t[:, first * line:last * line], rows, preferred_element_type=F32)

    out_ref[...] = (blend(0, SIDE - 2) + blend(SIDE - 2, SIDE)).astype(BF16)

    total_of(lists.at[pl.ds(0, n_row - 1)], list_send).wait()
    total_of(send_aux.at[pl.ds(0, SIDE - 1)], aux_send).wait()
    total_of(new_all.at[pl.ds(0, SIDE - 1)], new_send).wait()
    total_of(codes.at[pl.ds(0, SIDE - 1)], code_send).wait()
    total_of(got_emb.at[pl.ds(0, n_row - 1)], emb_send).wait()
    total_of(met.at[pl.ds(0, SIDE - 1)], met_send).wait()
    total_of(parts, part_send).wait()


def solution(mesh):
    n_row, n_col = mesh.shape["row"], mesh.shape["col"]

    def local(new_aux, former_auxiliary_rows, old_emb, neighbour_ids, neighbour_counts):
        new_dev, width = new_aux.shape
        old_dev = former_auxiliary_rows.shape[0]
        slots_row = neighbour_ids.shape[1]
        slots = n_row * DISTINCT
        his = old_dev // LANES
        vm = pltpu.VMEM
        dma = pltpu.SemaphoreType.DMA
        hbm = pl.BlockSpec(memory_space=pl.ANY)
        return pl.pallas_call(
            functools.partial(kernel, n_row, n_col),
            out_shape=jax.ShapeDtypeStruct((new_dev, width), BF16),
            in_specs=[hbm] * 5,
            out_specs=pl.BlockSpec(memory_space=vm),
            scratch_shapes=[
                vm((slots_row, new_dev), I32), vm((1, new_dev), I32), vm((SIDE, new_dev, width), BF16),
                vm((old_dev, width), BF16), vm((old_dev, width), BF16),
                vm((his * n_row, slots_row * new_dev), BF16), vm((LANES, slots_row * new_dev), BF16),
                vm((his * n_row, LANES), F32), vm((n_row, 1, LANES), F32), vm((SIDE, SIDE, 1, LANES), F32),
                vm((slots, old_dev), BF16),
                vm((SIDE, SIDE, DISTINCT, width), BF16), vm((SIDE, SIDE, DISTINCT, width), BF16),
                vm((SIDE, SIDE, DISTINCT, width), BF16), vm((n_row, DISTINCT, width), BF16),
                vm((slots_row, new_dev), I32), vm((SIDE, slots_row, new_dev), I32),
                vm((slots_row, 8, new_dev), I32), vm((slots_row, 8, new_dev), F32),
                vm((slots, new_dev), F32),
                vm((SIDE, 2 * slots_row, new_dev), F32), vm((SIDE, 2 * slots_row, new_dev), F32),
                vm((2 * slots_row + 8, new_dev), F32), vm((n_col - 1, 2 * slots_row + 8, new_dev), F32),
                dma((5,)), dma(()), dma((SIDE,)), dma(()), dma((SIDE,)), dma(()), dma(()), dma(()), dma(()),
                dma(()), dma((SIDE,)), dma(()), dma(()), dma(()), dma(()),
            ],
            compiler_params=pltpu.CompilerParams(
                collective_id=0, has_side_effects=True, vmem_limit_bytes=67043328),
        )(neighbour_ids.T, neighbour_counts.reshape(1, new_dev), new_aux, former_auxiliary_rows, old_emb)

    return jax.shard_map(
        local,
        mesh=mesh,
        in_specs=(P("row", "col"), P("row", "col"), P("row", "col"), P("row", None), P("row")),
        out_specs=P("row", "col"),
        check_vma=False,
    )
```
